256 devices in a mesh: region: 16 (over x, y_lo, core), patch: 16 (over z, y_hi).
Axes of the slice: x: 4, y: 4 (y_hi: 2, y_lo: 2; y = y_hi * 2 + y_lo), z: 8, core: 2. Of those that a mesh axis runs over, the one named last changes fastest.
Arguments:
- nodes: bfloat16 [65536, 512], P(('region', 'patch')), may hold values from -6 to 6
- edges: bfloat16 [524288, 512], P(('region', 'patch')), may hold values from -6 to 6
- senders: int32 [524288], P(('region', 'patch')), may hold values from 0 to 799, as said below
- receivers: int32 [524288], P(('region', 'patch')), may hold values from 0 to 767, as said below
- valid_counts: int32 [256], P(('region', 'patch')), may hold values from 512 to 2048, as said below
- hub_owner: int32 [2, 16], P(None, 'region'), may hold values from 0 to 15
- edge_in: bfloat16 [2, 3, 512, 512], replicated, may hold values from -0.15625 to 0.15625
- edge_bias: float32 [2, 512], replicated, may hold values from -3 to 3
- edge_out: bfloat16 [2, 512, 512], replicated, may hold values from -0.25 to 0.25
- edge_gain: float32 [2, 512], replicated, may hold values from 0.25 to 1.75
- edge_shift: float32 [2, 512], replicated, may hold values from -2 to 2
- node_in: bfloat16 [2, 2, 512, 512], replicated, may hold values from -0.1875 to 0.1875
- node_bias: float32 [2, 512], replicated, may hold values from -3 to 3
- node_out: bfloat16 [2, 512, 512], replicated, may hold values from -0.25 to 0.25
- node_gain: float32 [2, 512], replicated, may hold values from 0.25 to 1.75
- node_shift: float32 [2, 512], replicated, may hold values from -2 to 2
Outputs:
- nodes_out: bfloat16 [65536, 512], P(('region', 'patch'))
- edges_out: bfloat16 [524288, 512], P(('region', 'patch'))
The draws below stay inside these ranges and needn't reach their ends.
Inputs may be any that keep to these rules, and one draw needn't show every extreme that they name: `senders`: codes below 256 name a row of the previous patch, below 512 of the own patch, below 768 of the next patch, the rest a hub row. `receivers`: codes below 256 name a row of the previous patch, below 512 of the own patch, the rest of the next patch. `valid_counts`: live slots are the first ones of a patch; some patch has all 2048 slots live.
All inputs are finite; a program needn't handle non-finite values.
Results may differ from the reference program's by a relative error of at most 0.012.
Values may be sent and summed in bfloat16 or wider, within the bound.
A program may use at most 64 MiB of HBM per device.

```python
import jax
import jax.numpy as jnp
from jax import lax

D = 512
NODE_DEV = 256
EDGE_DEV = 2048
HUB = 32
LAYERS = 2
NODES = 65536
EDGES = 524288
N_REGION = 16
N_PATCH = 16


def draw_senders(key, part):
    kinds = jax.random.randint(jax.random.fold_in(key, 11), (EDGES,), 0, 20)
    offset = jax.random.randint(jax.random.fold_in(key, 12), (EDGES,), 0, NODE_DEV)
    hub_pick = jax.random.randint(jax.random.fold_in(key, 13), (EDGES,), 0, HUB)
    codes = jnp.where(kinds < 4, offset, jnp.where(kinds < 10, NODE_DEV + offset, jnp.where(kinds < 14, 2 * NODE_DEV + offset, 3 * NODE_DEV + hub_pick)))
    return codes.astype(jnp.int32)


def draw_receivers(key, part):
    kinds = jax.random.randint(jax.random.fold_in(key, 21), (EDGES,), 0, 16)
    offset = jax.random.randint(jax.random.fold_in(key, 22), (EDGES,), 0, NODE_DEV)
    codes = jnp.where(kinds < 4, offset, jnp.where(kinds < 12, NODE_DEV + offset, 2 * NODE_DEV + offset))
    return codes.astype(jnp.int32)


def draw_valid_counts(key, part):
    total = N_REGION * N_PATCH
    counts = jax.random.randint(jax.random.fold_in(key, 31), (total,), EDGE_DEV // 4, EDGE_DEV + 1)
    fullest = jax.random.randint(jax.random.fold_in(key, 32), (), 0, total)
    return jnp.where(jnp.arange(total) == fullest, EDGE_DEV, counts).astype(jnp.int32)


def touch_ends(drawn, own_key, least, high):
    dims = drawn.shape
    spot = [jax.random.randint(jax.random.fold_in(own_key, axis), (), 0, dims[axis]) for axis in range(len(dims))]
    drawn = drawn.at[tuple(spot)].set(least)
    longest = dims.index(max(dims))
    spot[longest] = (spot[longest] + 1) % dims[longest]
    return drawn.at[tuple(spot)].set(high)


def level_of(stream_key, extent, pieces, least, largest):
    factor_of = 1.0
    for dim, parts in pieces:
        heights = jax.random.uniform(jax.random.fold_in(jax.random.fold_in(stream_key, 6), dim), (parts,), jnp.float32, least / len(pieces), largest / len(pieces))
        factor_of = factor_of * jnp.repeat(jnp.exp(heights), extent[dim] // parts).reshape((-1,) + (1,) * (len(extent) - 1 - dim))
    return factor_of


def scatter_about(own_key, extent, scale, reach, shards=(), kind=jnp.bfloat16):
    result = jax.random.normal(own_key, extent, jnp.float32) * scale
    if len(shards) > 0:
        result = level_of(own_key, extent, shards, -0.22, 0.18) * result
    return jnp.clip(result, min=-reach, max=reach).astype(kind)


def setup_inputs(seed: int = 0) -> dict:
    key_of = jax.random.split(jax.random.key(seed), 17)
    return {
        "nodes": scatter_about(key_of[0], (NODES, D), 1.0, 6.0, ((0, 256),)),
        "edges": scatter_about(key_of[1], (EDGES, D), 1.0, 6.0, ((0, 256),)),
        "senders": draw_senders(jax.random.fold_in(key_of[16], 71), 0),
        "receivers": draw_receivers(jax.random.fold_in(key_of[16], 71), 0),
        "valid_counts": draw_valid_counts(jax.random.fold_in(key_of[16], 71), 0),
        "hub_owner": touch_ends(jax.random.randint(key_of[5], (LAYERS, N_REGION), 0, N_PATCH), jax.random.fold_in(key_of[5], 1), 0, N_PATCH - 1).astype(jnp.int32),
        "edge_in": scatter_about(key_of[6], (LAYERS, 3, D, D), (3 * D) ** -0.5, 0.15625),
        "edge_bias": scatter_about(key_of[7], (LAYERS, D), 0.5, 3.0, (), jnp.float32),
        "edge_out": scatter_about(key_of[8], (LAYERS, D, D), D ** -0.5, 0.25),
        "edge_gain": jnp.clip(1.0 + 0.15 * jax.random.normal(key_of[9], (LAYERS, D), jnp.float32), 0.25, 1.75),
        "edge_shift": scatter_about(key_of[10], (LAYERS, D), 0.3, 2.0, (), jnp.float32),
        "node_in": scatter_about(key_of[11], (LAYERS, 2, D, D), (2 * D) ** -0.5, 0.1875),
        "node_bias": scatter_about(key_of[12], (LAYERS, D), 0.5, 3.0, (), jnp.float32),
        "node_out": scatter_about(key_of[13], (LAYERS, D, D), D ** -0.5, 0.25),
        "node_gain": jnp.clip(1.0 + 0.15 * jax.random.normal(key_of[14], (LAYERS, D), jnp.float32), 0.25, 1.75),
        "node_shift": scatter_about(key_of[15], (LAYERS, D), 0.3, 2.0, (), jnp.float32),
    }


epsilon = 1e-05

def activate(value):
    return value / (1.0 + jnp.exp(-value))

def layer_norm(value, gain, shift):
    center = value - lax.optimization_barrier(jnp.mean(value, axis=-1, keepdims=True))
    spread = lax.optimization_barrier(jnp.mean(center * center, axis=-1, keepdims=True))
    return center * lax.rsqrt(spread + epsilon) * gain + shift

def locate(codes, device_id, hub_device):
    region_id = device_id // N_PATCH
    patch_id = device_id % N_PATCH
    before_dev = region_id * N_PATCH + (patch_id + N_PATCH - 1) % N_PATCH
    after_dev = region_id * N_PATCH + (patch_id + 1) % N_PATCH
    found = jnp.where(codes < NODE_DEV, before_dev * NODE_DEV + codes, jnp.where(codes < 2 * NODE_DEV, device_id * NODE_DEV + codes - NODE_DEV, jnp.where(codes < 3 * NODE_DEV, after_dev * NODE_DEV + codes - 2 * NODE_DEV, hub_device * NODE_DEV + codes - 3 * NODE_DEV)))
    return found.astype(jnp.int32)

def reference(nodes, edges, senders, receivers, valid_counts, hub_owner, edge_in, edge_bias, edge_out, edge_gain, edge_shift, node_in, node_bias, node_out, node_gain, node_shift):
    positions = jnp.arange(EDGES, dtype=jnp.int32)
    device_id = (positions // EDGE_DEV).astype(jnp.int32)
    region_id = (device_id // N_PATCH).astype(jnp.int32)
    is_valid = positions % EDGE_DEV < jnp.take(valid_counts, device_id)
    recv_index = locate(receivers, device_id, device_id)
    for layer_index in range(LAYERS):
        hub_device = region_id * N_PATCH + jnp.take(hub_owner[layer_index], region_id)
        send_index = locate(senders, device_id, hub_device)
        send_proj = jnp.dot(nodes, edge_in[layer_index, 1], preferred_element_type=jnp.float32).astype(jnp.bfloat16)
        recv_proj = jnp.dot(nodes, edge_in[layer_index, 2], preferred_element_type=jnp.float32).astype(jnp.bfloat16)
        pre_edge = jnp.dot(edges, edge_in[layer_index, 0], preferred_element_type=jnp.float32)
        pre_edge = pre_edge + jnp.take(send_proj, send_index, axis=0).astype(jnp.float32)
        pre_edge = pre_edge + jnp.take(recv_proj, recv_index, axis=0).astype(jnp.float32)
        pre_edge = pre_edge + edge_bias[layer_index]
        activated = activate(pre_edge).astype(jnp.bfloat16)
        mixed = jnp.dot(activated, edge_out[layer_index], preferred_element_type=jnp.float32)
        updated = edges.astype(jnp.float32) + layer_norm(mixed, edge_gain[layer_index], edge_shift[layer_index])
        edges = jnp.where(is_valid[:, None], updated, 0.0).astype(jnp.bfloat16)
        aggregate = jax.ops.segment_sum(edges.astype(jnp.float32), recv_index, num_segments=NODES).astype(jnp.bfloat16)
        pre_node = jnp.dot(nodes, node_in[layer_index, 0], preferred_element_type=jnp.float32)
        pre_node = pre_node + jnp.dot(aggregate, node_in[layer_index, 1], preferred_element_type=jnp.float32)
        pre_node = pre_node + node_bias[layer_index]
        node_act = activate(pre_node).astype(jnp.bfloat16)
        node_mixed = jnp.dot(node_act, node_out[layer_index], preferred_element_type=jnp.float32)
        nodes = (nodes.astype(jnp.float32) + layer_norm(node_mixed, node_gain[layer_index], node_shift[layer_index])).astype(jnp.bfloat16)
    return (nodes, edges)
```

```python
import functools

import jax
import jax.numpy as jnp
from jax import lax
from jax.experimental import pallas as pl
from jax.experimental.pallas import tpu as pltpu
from jax.sharding import PartitionSpec as P

HUB = 32
LAYERS = 2
GROUPS = ("region", "patch")
N_PATCH = 16
MESH = pl.DeviceIdType.MESH
EPS = 1e-05
TILE = 256
CHUNKS = 8
PIECES = 4
HUB_STAGES = ((1, 2, 3), (4, 8, 12))


def flipped(index, mask):
    for bit in (1, 2, 4, 8):
        if mask & bit:
            index = index + bit - 2 * bit * ((index // bit) % 2)
    return index


def silu(value):
    half = 0.5 * value
    return half + half * jnp.tanh(half)


def normed(value, gain, shift):
    center = value - jnp.mean(value, axis=-1, keepdims=True)
    spread = jnp.mean(center * center, axis=-1, keepdims=True)
    return center * lax.rsqrt(spread + EPS) * gain + shift


def mm(a, b):
    return jnp.dot(a, b, preferred_element_type=jnp.float32)


def kernel(
    nodes_hbm, edges_hbm, send_codes, recv_codes, valid_counts, hub_owner,
    ein_hbm, ebias, eout_hbm, egain, eshift, nin_hbm, nbias, nout_hbm, ngain, nshift,
    nodes_out, edges_out,
    hself, hpart, hfar, edges, pre, onehot, scatter, table,
    ein, eout, nin, nout,
    sum_self, sum_part, sum_far,
    hub_own, hub_first, hub_mid, hub_second,
    fub_own, fub_first, fub_mid, fub_second,
    self_send, self_in, far_send, far_in, back_send, back_in, pass_send, pass_in,
    far_send2, far_in2, back_send2, back_in2,
    local_sems, send_sems, recv_sems,
):
    rows = hself.shape[0]
    dim = hself.shape[1]
    count = edges.shape[0]
    tiles = count // TILE
    bf16 = jnp.bfloat16
    me = lax.axis_index("patch")
    region = lax.axis_index("region")
    odd = me % 2
    part = me + 1 - 2 * odd
    onward = (me + 2 - 4 * odd + N_PATCH) % N_PATCH
    source = (me - 2 + 4 * odd + N_PATCH) % N_PATCH
    far = (me - 1 + 2 * odd + N_PATCH) % N_PATCH

    barrier = pltpu.get_barrier_semaphore()
    greeted = [part, onward, source] + [flipped(me, m) for s in HUB_STAGES for m in s if m != 1]
    for other in greeted:
        pl.semaphore_signal(barrier, inc=1, device_id=(region, other), device_id_type=MESH)

    def load(src, dst, index):
        copy = pltpu.make_async_copy(src, dst, local_sems.at[index])
        copy.start()
        return copy

    get_nodes = load(nodes_hbm, hself, 0)
    get_ein0 = load(ein_hbm.at[0], ein.at[0], 1)
    get_edges = load(edges_hbm, edges, 2)
    get_eout = load(eout_hbm, eout, 3)
    get_nin = load(nin_hbm, nin, 4)
    get_nout = load(nout_hbm, nout, 5)
    get_ein1 = load(ein_hbm.at[1], ein.at[1], 6)

    used = [0]

    def send(src, dst, other):
        index = used[0]
        used[0] += 1
        copy = pltpu.make_async_remote_copy(
            src, dst, send_sems.at[index], recv_sems.at[index],
            device_id=(region, other), device_id_type=MESH,
        )
        copy.start()
        return copy

    sent = []

    codes = send_codes[...]
    is_odd = odd == 1
    behind = jnp.where(is_odd, codes + 2 * rows, codes + 4 * rows)
    ahead = jnp.where(is_odd, codes + 2 * rows, codes)
    send_pos = jnp.where(
        codes < rows, behind,
        jnp.where(codes < 2 * rows, codes - rows, jnp.where(codes < 3 * rows, ahead, codes + 3 * rows)),
    )
    rcodes = recv_codes[...]
    behind = jnp.where(is_odd, rcodes + 3 * rows, rcodes + 5 * rows)
    ahead = jnp.where(is_odd, rcodes + 3 * rows, rcodes + rows)
    recv_pos = jnp.where(rcodes < rows, behind, jnp.where(rcodes < 2 * rows, rcodes, ahead))
    behind = jnp.where(is_odd, rcodes + rows, rcodes + 2 * rows)
    ahead = jnp.where(is_odd, rcodes, rcodes - rows)
    add_pos = jnp.where(rcodes < rows, behind, jnp.where(rcodes < 2 * rows, rcodes - rows, ahead))
    block = 128
    lane = lax.broadcasted_iota(jnp.int32, (block, block), 1)
    line = lax.broadcasted_iota(jnp.int32, (3 * rows, block), 0)
    hub_at = 6 * rows
    width = rows // block
    for b in range(count // block):
        send_col = jnp.broadcast_to(send_pos[b : b + 1, :], (block, block)).T
        recv_col = jnp.broadcast_to(recv_pos[b : b + 1, :], (block, block)).T
        for seg in range(7):
            for w in range(width if seg < 6 else 1):
                start = seg * rows + w * block
                col = send_col if seg % 2 == 0 else recv_col
                onehot[b * block : (b + 1) * block, start : start + block] = jnp.where(
                    col == lane + start, 1.0, 0.0
                ).astype(bf16)
        scatter[:, b * block : (b + 1) * block] = jnp.where(
            add_pos[b : b + 1, :] == line, 1.0, 0.0
        ).astype(bf16)
    table[hub_at:, :] = jnp.zeros((block, dim), bf16)

    get_nodes.wait()
    head = hself[0:HUB, :]
    owner0 = hub_owner[0, 0]
    owner1 = hub_owner[1, 0]
    zero_head = jnp.zeros_like(head)
    hub_own[0:HUB, :] = jnp.where(owner0 == me, head, zero_head)
    hub_own[HUB:, :] = jnp.where(owner1 == me, head, zero_head)

    pl.semaphore_wait(barrier, len(greeted))

    def hub_start(src, dst, stage):
        return [send(src, dst.at[j], flipped(me, m)) for j, m in enumerate(HUB_STAGES[stage])]

    def hub_sum(own, got):
        total = own[...].astype(jnp.float32)
        for j in range(3):
            total = total + got[j].astype(jnp.float32)
        return total.astype(bf16)

    step = rows // CHUNKS
    out_part = [
        send(hself.at[pl.ds(i * step, step)], hpart.at[pl.ds(i * step, step)], part)
        for i in range(CHUNKS)
    ]
    hub_a = hub_start(hub_own, hub_first, 0)
    sent += hub_a

    def project(layer, start, h):
        table[start : start + rows, :] = mm(h, ein[layer, 1]).astype(bf16)
        table[start + rows : start + 2 * rows, :] = mm(h, ein[layer, 2]).astype(bf16)

    def project_hub(layer, h):
        table[hub_at : hub_at + HUB, :] = mm(h, ein[layer, 1]).astype(bf16)

    def tile_at(t):
        return pl.ds(pl.multiple_of(t * TILE, TILE), TILE)

    def gather(low, high):
        def body(t, carry):
            at = tile_at(t)
            pre[at, :] += mm(onehot[at, low:high], table[low:high, :])
            return carry

        lax.fori_loop(0, tiles, body, 0)

    def update_edges(layer, low, high):
        valid = valid_counts[0]
        gain = egain[layer : layer + 1, :]
        shift = eshift[layer : layer + 1, :]

        def body(t, carry):
            at = tile_at(t)
            total = pre[at, :] + mm(onehot[at, low:high], table[low:high, :])
            mixed = mm(silu(total).astype(bf16), eout[layer])
            updated = edges[at, :].astype(jnp.float32) + normed(mixed, gain, shift)
            row = lax.broadcasted_iota(jnp.int32, (TILE, 1), 0) + t * TILE
            edges[at, :] = jnp.where(row < valid, updated, 0.0).astype(bf16)
            if layer == LAYERS - 1:
                pltpu.make_async_copy(edges.at[at], edges_out.at[at], local_sems.at[7]).start()
            return carry

        lax.fori_loop(0, tiles, body, 0)

    def update_nodes(layer, h, aggregate):
        total = mm(h, nin[layer, 0]) + mm(aggregate, nin[layer, 1]) + nbias[layer : layer + 1, :]
        mixed = mm(silu(total).astype(bf16), nout[layer])
        gain = ngain[layer : layer + 1, :]
        shift = nshift[layer : layer + 1, :]
        return (h.astype(jnp.float32) + normed(mixed, gain, shift)).astype(bf16)

    def edge_part(layer, own):
        bias = ebias[layer : layer + 1, :]

        def body(t, carry):
            at = tile_at(t)
            total = mm(edges[at, :], ein[layer, 0]) + bias
            if own:
                total = total + mm(onehot[at, 0 : 2 * rows], table[0 : 2 * rows, :])
            pre[at, :] = total
            return carry

        lax.fori_loop(0, tiles, body, 0)

    get_ein0.wait()
    project(0, 0, hself[...])
    get_edges.wait()
    edge_part(0, True)
    out_far = []
    for i in range(CHUNKS):
        out_part[i].wait_recv()
        out_far.append(
            send(hpart.at[pl.ds(i * step, step)], hfar.at[pl.ds(i * step, step)], onward)
        )
        if i == CHUNKS // 2:
            for copy in hub_a:
                copy.wait_recv()
            hub_mid[...] = hub_sum(hub_own, hub_first)
            hub_b = hub_start(hub_mid, hub_second, 1)
    passed = out_far
    sent += hub_b
    project(0, 2 * rows, hpart[...])
    gather(2 * rows, 4 * rows)
    for copy in hub_b:
        copy.wait_recv()
    hub_all = hub_sum(hub_mid, hub_second)
    project_hub(0, hub_all[0:HUB, :])
    for copy in out_far:
        copy.wait_recv()
    project(0, 4 * rows, hfar[...])
    get_eout.wait()
    update_edges(0, 4 * rows, hub_at + block)

    size = rows // PIECES
    values = mm(scatter[0:rows, :], edges[...])
    sum_self[...] = values
    self_send[...] = values.astype(bf16)
    values = mm(scatter[2 * rows : 3 * rows, :], edges[...])
    out_self = [
        send(self_send.at[pl.ds(i * size, size)], self_in.at[pl.ds(i * size, size)], part)
        for i in range(PIECES)
    ]
    sum_far[...] = values
    far_send[...] = values.astype(bf16)
    sum_part[...] = mm(scatter[rows : 2 * rows, :], edges[...])
    out_far = [
        send(far_send.at[pl.ds(i * size, size)], far_in.at[pl.ds(i * size, size)], source)
        for i in range(PIECES)
    ]
    zero_sum = jnp.zeros((HUB, dim), jnp.float32)
    fub_own[...] = (
        jnp.where(owner1 == me, sum_self[0:HUB, :], zero_sum)
        + jnp.where(owner1 == part, sum_part[0:HUB, :], zero_sum)
        + jnp.where(owner1 == far, sum_far[0:HUB, :], zero_sum)
    ).astype(bf16)
    get_ein1.wait()
    edge_part(1, False)
    hub_a = hub_start(fub_own, fub_first, 0)
    sent += out_self + out_far + hub_a
    out_back = []
    out_pass = []
    for i in range(PIECES):
        at = pl.ds(i * size, size)
        mine = sum_part[at, :]
        out_far[i].wait_recv()
        from_far = far_in[at, :].astype(jnp.float32)
        back_send[at, :] = (mine + from_far).astype(bf16)
        out_self[i].wait_recv()
        from_part = self_in[at, :].astype(jnp.float32)
        pass_send[at, :] = (mine + from_part).astype(bf16)
        sum_part[at, :] = mine + from_far + from_part
        out_back.append(send(back_send.at[at], back_in.at[at], part))
        out_pass.append(send(pass_send.at[at], pass_in.at[at], onward))
    for copy in hub_a:
        copy.wait_recv()
    fub_mid[...] = hub_sum(fub_own, fub_first)
    get_nin.wait()
    get_nout.wait()
    for copy in passed:
        copy.wait_send()
    hpart[...] = update_nodes(0, hpart[...], sum_part[...].astype(bf16))
    hub_b = hub_start(fub_mid, fub_second, 1)
    sent += out_back + out_pass + hub_b
    project(1, 2 * rows, hpart[...])
    gather(2 * rows, 4 * rows)
    for copy in out_pass:
        copy.wait_recv()
    hfar_new = update_nodes(
        0, hfar[...], (sum_far[...] + pass_in[...].astype(jnp.float32)).astype(bf16)
    )
    project(1, 4 * rows, hfar_new)
    for copy in hub_b:
        copy.wait_recv()
    hub_new = update_nodes(0, hub_all[HUB:, :], hub_sum(fub_mid, fub_second))
    project_hub(1, hub_new)
    gather(4 * rows, hub_at + block)
    for copy in out_back:
        copy.wait_recv()
    hown = update_nodes(
        0, hself[...], (sum_self[...] + back_in[...].astype(jnp.float32)).astype(bf16)
    )
    project(1, 0, hown)
    update_edges(1, 0, 2 * rows)

    values = mm(scatter[2 * rows : 3 * rows, :], edges[...])
    far_send2[...] = values.astype(bf16)
    sum_part[...] = mm(scatter[rows : 2 * rows, :], edges[...])
    out_far = [
        send(far_send2.at[pl.ds(i * size, size)], far_in2.at[pl.ds(i * size, size)], source)
        for i in range(PIECES)
    ]
    sum_self[...] = mm(scatter[0:rows, :], edges[...])
    out_back = []
    for i in range(PIECES):
        at = pl.ds(i * size, size)
        out_far[i].wait_recv()
        back_send2[at, :] = (sum_part[at, :] + far_in2[at, :].astype(jnp.float32)).astype(bf16)
        out_back.append(send(back_send2.at[at], back_in2.at[at], part))
    sent += out_far + out_back
    for copy in out_back:
        copy.wait_recv()
    for copy in out_part:
        copy.wait_send()
    hself[...] = update_nodes(
        1, hown, (sum_self[...] + back_in2[...].astype(jnp.float32)).astype(bf16)
    )
    put = pltpu.make_async_copy(hself, nodes_out, local_sems.at[8])
    put.start()
    for copy in sent:
        copy.wait_send()
    put.wait()
    pltpu.make_async_copy(edges, edges_out, local_sems.at[7]).wait()


def local(
    nodes, edges, senders, receivers, valid_counts, hub_owner, edge_in, edge_bias, edge_out, edge_gain,
    edge_shift, node_in, node_bias, node_out, node_gain, node_shift,
):
    rows, dim = nodes.shape
    count = edges.shape[0]
    bf16 = jnp.bfloat16
    senders = senders.reshape(count // 128, 128)
    receivers = receivers.reshape(count // 128, 128)
    hbm = pl.BlockSpec(memory_space=pl.ANY)
    vmem = pl.BlockSpec(memory_space=pltpu.VMEM)
    smem = pl.BlockSpec(memory_space=pltpu.SMEM)
    block = pltpu.VMEM((rows, dim), bf16)
    total = pltpu.VMEM((rows, dim), jnp.float32)
    hub = pltpu.VMEM((2 * HUB, dim), bf16)
    hub3 = pltpu.VMEM((3, 2 * HUB, dim), bf16)
    fub = pltpu.VMEM((HUB, dim), bf16)
    fub3 = pltpu.VMEM((3, HUB, dim), bf16)
    places = 6 * rows + 128
    return pl.pallas_call(
        kernel,
        out_shape=(
            jax.ShapeDtypeStruct((rows, dim), bf16),
            jax.ShapeDtypeStruct((count, dim), bf16),
        ),
        in_specs=[hbm, hbm, vmem, vmem, smem, smem, hbm, vmem, hbm, vmem, vmem, hbm, vmem, hbm, vmem, vmem],
        out_specs=(hbm, hbm),
        scratch_shapes=[
            block, block, block,
            pltpu.VMEM((count, dim), bf16),
            pltpu.VMEM((count, dim), jnp.float32),
            pltpu.VMEM((count, places), bf16),
            pltpu.VMEM((3 * rows, count), bf16),
            pltpu.VMEM((places, dim), bf16),
            pltpu.VMEM(edge_in.shape, bf16),
            pltpu.VMEM(edge_out.shape, bf16),
            pltpu.VMEM(node_in.shape, bf16),
            pltpu.VMEM(node_out.shape, bf16),
            total, total, total,
            hub, hub3, hub, hub3,
            fub, fub3, fub, fub3,
            block, block, block, block, block, block, block, block,
            block, block, block, block,
            pltpu.SemaphoreType.DMA((9,)),
            pltpu.SemaphoreType.DMA((64,)),
            pltpu.SemaphoreType.DMA((64,)),
        ],
        compiler_params=pltpu.CompilerParams(
            collective_id=0, has_side_effects=True, vmem_limit_bytes=60 * 1024 * 1024
        ),
        name="steps",
    )(
        nodes, edges, senders, receivers, valid_counts, hub_owner, edge_in, edge_bias, edge_out,
        edge_gain, edge_shift, node_in, node_bias, node_out, node_gain, node_shift,
    )


def solution(mesh):
    split = P(GROUPS, None)
    line = P(GROUPS)
    return jax.shard_map(
        local,
        mesh=mesh,
        in_specs=(split, split, line, line, line, P(None, "region")) + (P(),) * 10,
        out_specs=(split, split),
        check_vma=False,
    )
```

```python
import functools

import jax
import jax.numpy as jnp
from jax import lax
from jax.experimental import pallas as pl
from jax.experimental.pallas import tpu as pltpu
from jax.sharding import PartitionSpec as P

HUB = 32
LAYERS = 2
GROUPS = ("region", "patch")
N_PATCH = 16
RUN = N_PATCH // 2
HUB_TURN = 3
FUB_TURN = 2
HUB_AT = 1024
OWN = 1152
PLACES = 1664
MESH = pl.DeviceIdType.MESH
EPS = 1e-05
TILE = 256
CHUNKS = 8
PIECES = 4


def flipped(index, mask):
    for bit in (1, 2, 4, 8):
        if mask & bit:
            index = index + bit - 2 * bit * ((index // bit) % 2)
    return index


class Trip:
    def __init__(self, copy):
        self.copy, self.left, self.landed = copy, False, False

    def wait_send(self):
        if not self.left:
            self.copy.wait_send()
        self.left = True

    def wait_recv(self):
        if not self.landed:
            self.copy.wait_recv()
        self.landed = True


def silu(half):
    return half + half * jnp.tanh(half)


def normed(value, gain, shift):
    share = 1.0 / value.shape[-1]
    center = value - jnp.sum(value, axis=-1, keepdims=True) * share
    spread = jnp.sum(center * center, axis=-1, keepdims=True) * share
    return center * lax.rsqrt(spread + EPS) * gain + shift


def mm(a, b):
    return jnp.dot(a, b, preferred_element_type=jnp.float32)


def kernel(
    nodes_hbm, edges_hbm, send_codes, recv_codes, valid_counts, hub_owner,
    ein_hbm, ebias, eout_hbm, egain, eshift, nin_hbm, nbias, nout_hbm, ngain, nshift,
    nodes_out, edges_out,
    hself, hpart, hfar, edges, pre, onehot, scatter, table,
    ein, eout, nin, nout,
    sum_self, sum_part, sum_far,
    hub_own, hub_got, hub_mid, hub_all, hub_rows,
    aux_own, aux_got, aux_mid, aux_all, aux_rows,
    fub_own, fub_got, fub_mid, fub_all, fub_rows,
    mixed_tile,
    self_send, self_in, far_send, far_in, back_send, back_in, pass_send, pass_in,
    far_send2, far_in2, back_send2, back_in2,
    local_sems, send_sems, recv_sems,
):
    rows = hself.shape[0]
    dim = hself.shape[1]
    count = edges.shape[0]
    tiles = count // TILE
    bf16 = jnp.bfloat16
    me = lax.axis_index("patch")
    region = lax.axis_index("region")
    odd = me % 2
    part = me + 1 - 2 * odd
    onward = (me + 2 - 4 * odd + N_PATCH) % N_PATCH
    source = (me - 2 + 4 * odd + N_PATCH) % N_PATCH
    far = (me - 1 + 2 * odd + N_PATCH) % N_PATCH

    barrier = pltpu.get_barrier_semaphore()
    others = [flipped(me, m) for m in range(1, N_PATCH)]
    greeted = [onward, source] + others
    for other in greeted:
        pl.semaphore_signal(barrier, inc=1, device_id=(region, other), device_id_type=MESH)

    def load(src, dst, index):
        copy = pltpu.make_async_copy(src, dst, local_sems.at[index])
        copy.start()
        return copy

    get_nodes = load(nodes_hbm, hself, 0)
    get_ein0 = load(ein_hbm.at[0], ein.at[0], 1)
    get_edges = load(edges_hbm, edges, 2)
    get_eout = load(eout_hbm, eout, 3)
    get_nin = load(nin_hbm, nin, 4)
    get_nout = load(nout_hbm, nout, 5)
    get_ein1 = load(ein_hbm.at[1], ein.at[1], 6)

    used = [0]

    def send(src, dst, other):
        index = used[0]
        used[0] += 1
        copy = pltpu.make_async_remote_copy(
            src, dst, send_sems.at[index], recv_sems.at[index],
            device_id=(region, other), device_id_type=MESH,
        )
        copy.start()
        trip = Trip(copy)
        sent.append(trip)
        return trip

    sent = []

    codes = send_codes[...]
    is_odd = odd == 1
    behind = jnp.where(is_odd, codes, codes + 2 * rows)
    ahead = jnp.where(is_odd, codes, codes - 2 * rows)
    own = codes - rows + OWN
    send_pos = jnp.where(
        codes < rows, behind,
        jnp.where(codes < 2 * rows, own, jnp.where(codes < 3 * rows, ahead, codes + rows)),
    )
    rcodes = recv_codes[...]
    behind = jnp.where(is_odd, rcodes + rows, rcodes + 3 * rows)
    ahead = jnp.where(is_odd, rcodes + rows, rcodes - rows)
    recv_pos = jnp.where(rcodes < rows, behind, jnp.where(rcodes < 2 * rows, rcodes + OWN, ahead))
    behind = jnp.where(is_odd, rcodes + rows, rcodes + 2 * rows)
    ahead = jnp.where(is_odd, rcodes, rcodes - rows)
    add_pos = jnp.where(rcodes < rows, behind, jnp.where(rcodes < 2 * rows, rcodes - rows, ahead))
    block = 128
    lane = lax.broadcasted_iota(jnp.int32, (block, block), 1)
    line = lax.broadcasted_iota(jnp.int32, (3 * rows, block), 0)
    width = rows // block
    for b in range(count // block):
        send_col = jnp.broadcast_to(send_pos[b : b + 1, :], (block, block)).T
        recv_col = jnp.broadcast_to(recv_pos[b : b + 1, :], (block, block)).T
        starts = (0, rows, 2 * rows, 3 * rows, OWN, OWN + rows, HUB_AT)
        for seg, first in enumerate(starts):
            for w in range(width if seg < 6 else 1):
                start = first + w * block
                col = send_col if seg % 2 == 0 else recv_col
                onehot[b * block : (b + 1) * block, start : start + block] = jnp.where(
                    col == lane + start, 1.0, 0.0
                ).astype(bf16)
        scatter[:, b * block : (b + 1) * block] = jnp.where(
            add_pos[b : b + 1, :] == line, 1.0, 0.0
        ).astype(bf16)
    table[HUB_AT:OWN, :] = jnp.zeros((block, dim), bf16)

    def hub_cut(own, value):
        for piece in range(N_PATCH):
            r, c = divmod(piece, dim // 128)
            own[piece // 2, piece % 2] = value[r * 8 : (r + 1) * 8, c * 128 : (c + 1) * 128]

    get_nodes.wait()
    head = hself[0:HUB, :]
    owner0 = hub_owner[0]
    owner1 = hub_owner[1]
    zero_head = jnp.zeros_like(head)
    hub_cut(hub_own, jnp.where(owner0 == me, head, zero_head))
    hub_cut(aux_own, jnp.where(owner1 == me, head, zero_head))

    pl.semaphore_wait(barrier, len(greeted))

    def hub_scatter(own, got):
        return [send(own.at[other // 2], got.at[m], other) for m, other in enumerate(others)]

    def hub_gather(trips, own, got, mid, everyone):
        total = own[me // 2].astype(jnp.float32)
        for m, trip in enumerate(trips):
            trip.wait_recv()
            total = total + got[m].astype(jnp.float32)
        total = total.astype(bf16)
        mid[0] = total
        everyone[me // 2] = total
        return [send(mid.at[0], everyone.at[me // 2], other) for other in others[1::2]]

    def hub_join(trips, everyone, joined):
        for trip in trips:
            trip.wait_recv()
        for piece in range(N_PATCH):
            r, c = divmod(piece, dim // 128)
            joined[r * 8 : (r + 1) * 8, c * 128 : (c + 1) * 128] = everyone[piece // 2, piece % 2]

    step = rows // CHUNKS
    hub_a = hub_scatter(hub_own, hub_got)
    out_part = [
        send(hself.at[pl.ds(i * step, step)], hpart.at[pl.ds(i * step, step)], part)
        for i in range(CHUNKS)
    ]

    def project(layer, start, h):
        table[start : start + rows, :] = (0.5 * mm(h, ein[layer, 1])).astype(bf16)
        table[start + rows : start + 2 * rows, :] = (0.5 * mm(h, ein[layer, 2])).astype(bf16)

    def project_hub(layer, h):
        table[HUB_AT : HUB_AT + HUB, :] = (0.5 * mm(h, ein[layer, 1])).astype(bf16)

    def tile_at(t):
        return pl.ds(pl.multiple_of(t * TILE, TILE), TILE)

    def gather(low, high):
        def body(t, carry):
            at = tile_at(t)
            pre[at, :] += mm(onehot[at, low:high], table[low:high, :])
            return carry

        lax.fori_loop(0, tiles, body, 0)

    def update_edges(layer, low, high):
        valid = valid_counts[0]
        gain = egain[layer : layer + 1, :]
        shift = eshift[layer : layer + 1, :]

        def collect(t):
            at = tile_at(t)
            pre[at, :] += mm(onehot[at, low:high], table[low:high, :])

        def mix(t):
            mixed_tile[...] = mm(silu(pre[tile_at(t), :]).astype(bf16), eout[layer])

        def finish(t):
            at = tile_at(t)
            updated = edges[at, :].astype(jnp.float32) + normed(mixed_tile[...], gain, shift)
            row = lax.broadcasted_iota(jnp.int32, (TILE, 1), 0) + t * TILE
            edges[at, :] = jnp.where(row < valid, updated, 0.0).astype(bf16)
            if layer == LAYERS - 1:
                pltpu.make_async_copy(edges.at[at], edges_out.at[at], local_sems.at[7]).start()

        def body(t, carry):
            finish(t - 1)
            mix(t)
            collect(t + 1)
            return carry

        collect(0)
        mix(0)
        collect(1)
        lax.fori_loop(1, tiles - 1, body, 0)
        finish(tiles - 2)
        mix(tiles - 1)
        finish(tiles - 1)

    def update_nodes(layer, h, aggregate):
        total = mm(h, nin[layer, 0]) + mm(aggregate, nin[layer, 1]) + nbias[layer : layer + 1, :]
        mixed = mm(silu(0.5 * total).astype(bf16), nout[layer])
        gain = ngain[layer : layer + 1, :]
        shift = nshift[layer : layer + 1, :]
        return (h.astype(jnp.float32) + normed(mixed, gain, shift)).astype(bf16)

    def edge_part(layer, own):
        bias = ebias[layer : layer + 1, :]

        def body(t, carry):
            at = tile_at(t)
            total = 0.5 * (mm(edges[at, :], ein[layer, 0]) + bias)
            if own:
                total = total + mm(onehot[at, OWN:PLACES], table[OWN:PLACES, :])
            pre[at, :] = total
            return carry

        lax.fori_loop(0, tiles, body, 0)

    get_ein0.wait()
    project(0, OWN, hself[...])
    get_edges.wait()
    edge_part(0, True)
    out_far = []
    for i in range(CHUNKS):
        out_part[i].wait_recv()
        out_far.append(
            send(hpart.at[pl.ds(i * step, step)], hfar.at[pl.ds(i * step, step)], onward)
        )
        if i == HUB_TURN:
            hub_b = hub_gather(hub_a, hub_own, hub_got, hub_mid, hub_all)
    passed = out_far
    aux_a = hub_scatter(aux_own, aux_got)
    project(0, 0, hpart[...])
    gather(0, 2 * rows)
    hub_join(hub_b, hub_all, hub_rows)
    project_hub(0, hub_rows[...])
    for copy in out_far:
        copy.wait_recv()
    project(0, 2 * rows, hfar[...])
    get_eout.wait()
    aux_b = hub_gather(aux_a, aux_own, aux_got, aux_mid, aux_all)
    update_edges(0, 2 * rows, OWN)

    size = rows // PIECES
    values = mm(scatter[0:rows, :], edges[...])
    self_send[...] = values.astype(bf16)
    sum_self[...] = values
    values = mm(scatter[2 * rows : 3 * rows, :], edges[...])

    def send_self(i):
        return send(self_send.at[pl.ds(i * size, size)], self_in.at[pl.ds(i * size, size)], part)

    out_self = [send_self(i) for i in range(PIECES // 2)]
    far_send[...] = values.astype(bf16)
    sum_far[...] = values
    sum_part[...] = mm(scatter[rows : 2 * rows, :], edges[...])
    out_far = [
        send(far_send.at[pl.ds(i * size, size)], far_in.at[pl.ds(i * size, size)], source)
        for i in range(PIECES)
    ]
    zero_sum = jnp.zeros((HUB, dim), jnp.float32)
    hub_part = (
        jnp.where(owner1 == me, sum_self[0:HUB, :], zero_sum)
        + jnp.where(owner1 == part, sum_part[0:HUB, :], zero_sum)
        + jnp.where(owner1 == far, sum_far[0:HUB, :], zero_sum)
    ).astype(bf16)
    hub_cut(fub_own, hub_part)
    get_ein1.wait()
    fub_a = hub_scatter(fub_own, fub_got)
    out_self += [send_self(i) for i in range(PIECES // 2, PIECES)]
    edge_part(1, False)
    out_back = []
    out_pass = []
    for i in range(PIECES):
        at = pl.ds(i * size, size)
        mine = sum_part[at, :]
        out_far[i].wait_recv()
        from_far = far_in[at, :].astype(jnp.float32)
        back_send[at, :] = (mine + from_far).astype(bf16)
        sum_part[at, :] = mine + from_far
        out_back.append(send(back_send.at[at], back_in.at[at], part))
        out_self[i].wait_recv()
        from_part = self_in[at, :].astype(jnp.float32)
        pass_send[at, :] = (mine + from_part).astype(bf16)
        sum_part[at, :] = sum_part[at, :] + from_part
        out_pass.append(send(pass_send.at[at], pass_in.at[at], onward))
        if i == FUB_TURN:
            fub_b = hub_gather(fub_a, fub_own, fub_got, fub_mid, fub_all)
    get_nin.wait()
    get_nout.wait()
    for copy in passed:
        copy.wait_send()
    hpart[...] = update_nodes(0, hpart[...], sum_part[...].astype(bf16))
    project(1, 0, hpart[...])
    gather(0, 2 * rows)
    for copy in out_pass:
        copy.wait_recv()
    hfar_new = update_nodes(
        0, hfar[...], (sum_far[...] + pass_in[...].astype(jnp.float32)).astype(bf16)
    )
    project(1, 2 * rows, hfar_new)
    gather(2 * rows, 4 * rows)
    hub_join(aux_b, aux_all, aux_rows)
    hub_join(fub_b, fub_all, fub_rows)
    project_hub(1, update_nodes(0, aux_rows[...], fub_rows[...]))
    for copy in out_back:
        copy.wait_recv()
    hown = update_nodes(
        0, hself[...], (sum_self[...] + back_in[...].astype(jnp.float32)).astype(bf16)
    )
    project(1, OWN, hown)
    update_edges(1, HUB_AT, PLACES)

    values = mm(scatter[2 * rows : 3 * rows, :], edges[...])
    far_send2[...] = values.astype(bf16)
    sum_part[...] = mm(scatter[rows : 2 * rows, :], edges[...])
    out_far = [
        send(far_send2.at[pl.ds(i * size, size)], far_in2.at[pl.ds(i * size, size)], source)
        for i in range(PIECES)
    ]
    sum_self[...] = mm(scatter[0:rows, :], edges[...])
    out_back = []
    for i in range(PIECES):
        at = pl.ds(i * size, size)
        out_far[i].wait_recv()
        back_send2[at, :] = (sum_part[at, :] + far_in2[at, :].astype(jnp.float32)).astype(bf16)
        out_back.append(send(back_send2.at[at], back_in2.at[at], part))
    for copy in out_back:
        copy.wait_recv()
    for copy in out_part:
        copy.wait_send()
    hself[...] = update_nodes(
        1, hown, (sum_self[...] + back_in2[...].astype(jnp.float32)).astype(bf16)
    )
    put = pltpu.make_async_copy(hself, nodes_out, local_sems.at[8])
    put.start()
    for copy in sent:
        copy.wait_send()
    put.wait()
    pltpu.make_async_copy(edges, edges_out, local_sems.at[7]).wait()


def copy_kernel(nodes, edges, nodes_out, edges_out, rows, lines, in_sems, out_sems):
    cut = lines.shape[0] // 4
    spans = [(nodes, nodes_out, rows, pl.ds(0, rows.shape[0]))]
    spans += [(edges, edges_out, lines, pl.ds(i * cut, cut)) for i in range(4)]
    gets = [
        pltpu.make_async_copy(src.at[at], held.at[at], in_sems.at[i])
        for i, (src, _, held, at) in enumerate(spans)
    ]
    puts = [
        pltpu.make_async_copy(held.at[at], dst.at[at], out_sems.at[i])
        for i, (_, dst, held, at) in enumerate(spans)
    ]
    for get in gets:
        get.start()
    for get, put in zip(gets, puts):
        get.wait()
        put.start()
    for put in puts:
        put.wait()


def copied(nodes, edges):
    hbm = pl.BlockSpec(memory_space=pl.ANY)
    return pl.pallas_call(
        copy_kernel,
        out_shape=(
            jax.ShapeDtypeStruct(nodes.shape, nodes.dtype),
            jax.ShapeDtypeStruct(edges.shape, edges.dtype),
        ),
        in_specs=[hbm, hbm],
        out_specs=(hbm, hbm),
        scratch_shapes=[
            pltpu.VMEM(nodes.shape, nodes.dtype),
            pltpu.VMEM(edges.shape, edges.dtype),
            pltpu.SemaphoreType.DMA((5,)),
            pltpu.SemaphoreType.DMA((5,)),
        ],
        compiler_params=pltpu.CompilerParams(vmem_limit_bytes=60 * 1024 * 1024),
        name="place",
    )(nodes, edges)


def local(
    nodes, edges, senders, receivers, valid_counts, hub_owner, edge_in, edge_bias, edge_out, edge_gain,
    edge_shift, node_in, node_bias, node_out, node_gain, node_shift,
):
    rows, dim = nodes.shape
    count = edges.shape[0]
    bf16 = jnp.bfloat16
    hub_owner = hub_owner.reshape(LAYERS)
    senders = senders.reshape(count // 128, 128)
    receivers = receivers.reshape(count // 128, 128)
    hbm = pl.BlockSpec(memory_space=pl.ANY)
    vmem = pl.BlockSpec(memory_space=pltpu.VMEM)
    smem = pl.BlockSpec(memory_space=pltpu.SMEM)
    block = pltpu.VMEM((rows, dim), bf16)
    total = pltpu.VMEM((rows, dim), jnp.float32)

    def hub(pieces):
        return pltpu.VMEM((pieces, 2, 8, 128), bf16)

    hub_set = (hub(RUN), hub(N_PATCH - 1), hub(1), hub(RUN), pltpu.VMEM((HUB, dim), bf16))
    places = PLACES
    out = pl.pallas_call(
        kernel,
        out_shape=(
            jax.ShapeDtypeStruct((rows, dim), bf16),
            jax.ShapeDtypeStruct((count, dim), bf16),
        ),
        in_specs=[hbm, hbm, vmem, vmem, smem, smem, hbm, vmem, hbm, vmem, vmem, hbm, vmem, hbm, vmem, vmem],
        out_specs=(hbm, hbm),
        scratch_shapes=[
            block, block, block,
            pltpu.VMEM((count, dim), bf16),
            pltpu.VMEM((count, dim), jnp.float32),
            pltpu.VMEM((count, places), bf16),
            pltpu.VMEM((3 * rows, count), bf16),
            pltpu.VMEM((places, dim), bf16),
            pltpu.VMEM(edge_in.shape, bf16),
            pltpu.VMEM(edge_out.shape, bf16),
            pltpu.VMEM(node_in.shape, bf16),
            pltpu.VMEM(node_out.shape, bf16),
            total, total, total,
            *hub_set,
            *hub_set,
            *hub_set,
            pltpu.VMEM((TILE, dim), jnp.float32),
            block, block, block, block, block, block, block, block,
            block, block, block, block,
            pltpu.SemaphoreType.DMA((9,)),
            pltpu.SemaphoreType.DMA((112,)),
            pltpu.SemaphoreType.DMA((112,)),
        ],
        compiler_params=pltpu.CompilerParams(
            collective_id=0, has_side_effects=True, vmem_limit_bytes=60 * 1024 * 1024
        ),
        name="steps",
    )(
        nodes, edges, senders, receivers, valid_counts, hub_owner, edge_in, edge_bias, edge_out,
        edge_gain, edge_shift, node_in, node_bias, node_out, node_gain, node_shift,
    )
    return copied(*out)


def solution(mesh):
    split = P(GROUPS, None)
    line = P(GROUPS)
    return jax.shard_map(
        local,
        mesh=mesh,
        in_specs=(split, split, line, line, line, P(None, "region")) + (P(),) * 10,
        out_specs=(split, split),
        check_vma=False,
    )
```

```python
import functools

import jax
import jax.numpy as jnp
from jax import lax
from jax.experimental import pallas as pl
from jax.experimental.pallas import tpu as pltpu
from jax.sharding import PartitionSpec as P

HUB = 32
LAYERS = 2
GROUPS = ("region", "patch")
N_PATCH = 16
RUN = N_PATCH // 2
HUB_TURN = 3
FUB_TURN = 5
HUB_AT = 1024
OWN = 1152
PLACES = 1664
MESH = pl.DeviceIdType.MESH
EPS = 1e-05
TILE = 256
CHUNKS = 8
PIECES = 8


def flipped(index, mask):
    for bit in (1, 2, 4, 8):
        if mask & bit:
            index = index + bit - 2 * bit * ((index // bit) % 2)
    return index


class Trip:
    def __init__(self, copy):
        self.copy, self.left, self.landed = copy, False, False

    def wait_send(self):
        if not self.left:
            self.copy.wait_send()
        self.left = True

    def wait_recv(self):
        if not self.landed:
            self.copy.wait_recv()
        self.landed = True


def silu(half):
    return half + half * jnp.tanh(half)


def normed(value, gain, shift):
    share = 1.0 / value.shape[-1]
    center = value - jnp.sum(value, axis=-1, keepdims=True) * share
    spread = jnp.sum(center * center, axis=-1, keepdims=True) * share
    return center * lax.rsqrt(spread + EPS) * gain + shift


def mm(a, b):
    return jnp.dot(a, b, preferred_element_type=jnp.float32)


def kernel(
    nodes_hbm, edges_hbm, send_hbm, recv_hbm, valid_hbm, owner_hbm,
    ein_hbm, ebias_hbm, eout_hbm, egain_hbm, eshift_hbm, nin_hbm, nbias_hbm, nout_hbm, ngain_hbm, nshift_hbm,
    nodes_out, edges_out,
    hself, hpart, hfar, edges, pre, onehot, scatter, table,
    ein, eout, nin, nout,
    sum_self, sum_part, sum_far,
    hub_own, hub_got, hub_mid, hub_all, hub_rows,
    aux_own, aux_got, aux_mid, aux_all, aux_rows,
    fub_own, fub_got, fub_mid, fub_all, fub_rows,
    mixed_tile,
    send_codes, recv_codes, ebias, egain, eshift, nbias, ngain, nshift, valid_counts, hub_owner,
    self_send, self_in, far_send, far_in, back_send, back_in, pass_send, pass_in,
    far_send2, far_in2, back_send2, back_in2,
    local_sems, send_sems, recv_sems,
):
    rows = hself.shape[0]
    dim = hself.shape[1]
    count = edges.shape[0]
    tiles = count // TILE
    bf16 = jnp.bfloat16
    me = lax.axis_index("patch")
    region = lax.axis_index("region")
    odd = me % 2
    part = me + 1 - 2 * odd
    onward = (me + 2 - 4 * odd + N_PATCH) % N_PATCH
    source = (me - 2 + 4 * odd + N_PATCH) % N_PATCH
    far = (me - 1 + 2 * odd + N_PATCH) % N_PATCH

    barrier = pltpu.get_barrier_semaphore()
    others = [flipped(me, m) for m in range(1, N_PATCH)]
    greeted = [onward, source] + others
    for other in greeted:
        pl.semaphore_signal(barrier, inc=1, device_id=(region, other), device_id_type=MESH)

    def load(src, dst, index):
        copy = pltpu.make_async_copy(src, dst, local_sems.at[index])
        copy.start()
        return copy

    get_nodes = load(nodes_hbm, hself, 0)
    get_codes = [load(send_hbm, send_codes, 9), load(recv_hbm, recv_codes, 10)]
    get_codes += [load(owner_hbm, hub_owner, 11)]
    get_ein0 = load(ein_hbm.at[0], ein.at[0], 1)
    get_edges = load(edges_hbm, edges, 2)
    vectors = (
        (ebias_hbm, ebias), (egain_hbm, egain), (eshift_hbm, eshift), (nbias_hbm, nbias),
        (ngain_hbm, ngain), (nshift_hbm, nshift), (valid_hbm, valid_counts),
    )
    get_vectors = [load(src, dst, 12 + i) for i, (src, dst) in enumerate(vectors)]
    get_eout = load(eout_hbm, eout, 3)
    get_nin = load(nin_hbm, nin, 4)
    get_nout = load(nout_hbm, nout, 5)
    get_ein1 = load(ein_hbm.at[1], ein.at[1], 6)

    used = [0]

    def send(src, dst, other):
        index = used[0]
        used[0] += 1
        copy = pltpu.make_async_remote_copy(
            src, dst, send_sems.at[index], recv_sems.at[index],
            device_id=(region, other), device_id_type=MESH,
        )
        copy.start()
        trip = Trip(copy)
        sent.append(trip)
        return trip

    sent = []

    for get in get_codes:
        get.wait()
    codes = send_codes[...]
    is_odd = odd == 1
    behind = jnp.where(is_odd, codes, codes + 2 * rows)
    ahead = jnp.where(is_odd, codes, codes - 2 * rows)
    own = codes - rows + OWN
    send_pos = jnp.where(
        codes < rows, behind,
        jnp.where(codes < 2 * rows, own, jnp.where(codes < 3 * rows, ahead, codes + rows)),
    )
    rcodes = recv_codes[...]
    behind = jnp.where(is_odd, rcodes + rows, rcodes + 3 * rows)
    ahead = jnp.where(is_odd, rcodes + rows, rcodes - rows)
    recv_pos = jnp.where(rcodes < rows, behind, jnp.where(rcodes < 2 * rows, rcodes + OWN, ahead))
    behind = jnp.where(is_odd, rcodes + rows, rcodes + 2 * rows)
    ahead = jnp.where(is_odd, rcodes, rcodes - rows)
    add_pos = jnp.where(rcodes < rows, behind, jnp.where(rcodes < 2 * rows, rcodes - rows, ahead))
    block = 128
    lane = lax.broadcasted_iota(jnp.int32, (block, block), 1)
    line = lax.broadcasted_iota(jnp.int32, (3 * rows, block), 0)
    width = rows // block
    for b in range(count // block):
        send_col = jnp.broadcast_to(send_pos[b : b + 1, :], (block, block)).T
        recv_col = jnp.broadcast_to(recv_pos[b : b + 1, :], (block, block)).T
        starts = (0, rows, 2 * rows, 3 * rows, OWN, OWN + rows, HUB_AT)
        for seg, first in enumerate(starts):
            for w in range(width if seg < 6 else 1):
                start = first + w * block
                col = send_col if seg % 2 == 0 else recv_col
                onehot[b * block : (b + 1) * block, start : start + block] = jnp.where(
                    col == lane + start, 1.0, 0.0
                ).astype(bf16)
        scatter[:, b * block : (b + 1) * block] = jnp.where(
            add_pos[b : b + 1, :] == line, 1.0, 0.0
        ).astype(bf16)
    table[HUB_AT:OWN, :] = jnp.zeros((block, dim), bf16)

    def hub_cut(own, value):
        for piece in range(N_PATCH):
            r, c = divmod(piece, dim // 128)
            own[piece // 2, piece % 2] = value[r * 8 : (r + 1) * 8, c * 128 : (c + 1) * 128]

    get_nodes.wait()
    head = hself[0:HUB, :]
    owner0 = hub_owner[0]
    owner1 = hub_owner[1]
    zero_head = jnp.zeros_like(head)
    hub_cut(hub_own, jnp.where(owner0 == me, head, zero_head))
    hub_cut(aux_own, jnp.where(owner1 == me, head, zero_head))

    pl.semaphore_wait(barrier, len(greeted))

    def hub_scatter(own, got):
        return [send(own.at[other // 2], got.at[m], other) for m, other in enumerate(others)]

    def hub_gather(trips, own, got, mid, everyone):
        total = own[me // 2].astype(jnp.float32)
        for m, trip in enumerate(trips):
            trip.wait_recv()
            total = total + got[m].astype(jnp.float32)
        total = total.astype(bf16)
        mid[0] = total
        everyone[me // 2] = total
        return [send(mid.at[0], everyone.at[me // 2], other) for other in others[1::2]]

    def hub_join(trips, everyone, joined):
        for trip in trips:
            trip.wait_recv()
        for piece in range(N_PATCH):
            r, c = divmod(piece, dim // 128)
            joined[r * 8 : (r + 1) * 8, c * 128 : (c + 1) * 128] = everyone[piece // 2, piece % 2]

    step = rows // CHUNKS
    hub_a = hub_scatter(hub_own, hub_got)
    out_part = [
        send(hself.at[pl.ds(i * step, step)], hpart.at[pl.ds(i * step, step)], part)
        for i in range(CHUNKS)
    ]
    aux_a = hub_scatter(aux_own, aux_got)

    def project(layer, start, h):
        table[start : start + rows, :] = (0.5 * mm(h, ein[layer, 1])).astype(bf16)
        table[start + rows : start + 2 * rows, :] = (0.5 * mm(h, ein[layer, 2])).astype(bf16)

    def project_hub(layer, h):
        table[HUB_AT : HUB_AT + HUB, :] = (0.5 * mm(h, ein[layer, 1])).astype(bf16)

    def tile_at(t):
        return pl.ds(pl.multiple_of(t * TILE, TILE), TILE)

    def gather(low, high):
        def body(t, carry):
            at = tile_at(t)
            pre[at, :] += mm(onehot[at, low:high], table[low:high, :])
            return carry

        lax.fori_loop(0, tiles, body, 0)

    def update_edges(layer, low, high):
        valid = valid_counts[0]
        gain = egain[layer : layer + 1, :]
        shift = eshift[layer : layer + 1, :]

        def collect(t):
            at = tile_at(t)
            pre[at, :] += mm(onehot[at, low:high], table[low:high, :])

        def mix(t):
            mixed_tile[...] = mm(silu(pre[tile_at(t), :]).astype(bf16), eout[layer])

        def finish(t):
            at = tile_at(t)
            updated = edges[at, :].astype(jnp.float32) + normed(mixed_tile[...], gain, shift)
            row = lax.broadcasted_iota(jnp.int32, (TILE, 1), 0) + t * TILE
            edges[at, :] = jnp.where(row < valid, updated, 0.0).astype(bf16)
            if layer == LAYERS - 1:
                pltpu.make_async_copy(edges.at[at], edges_out.at[at], local_sems.at[7]).start()

        def body(t, carry):
            finish(t - 1)
            mix(t)
            collect(t + 1)
            return carry

        collect(0)
        mix(0)
        collect(1)
        lax.fori_loop(1, tiles - 1, body, 0)
        finish(tiles - 2)
        mix(tiles - 1)
        finish(tiles - 1)

    def update_nodes(layer, h, aggregate):
        total = mm(h, nin[layer, 0]) + mm(aggregate, nin[layer, 1]) + nbias[layer : layer + 1, :]
        mixed = mm(silu(0.5 * total).astype(bf16), nout[layer])
        gain = ngain[layer : layer + 1, :]
        shift = nshift[layer : layer + 1, :]
        return (h.astype(jnp.float32) + normed(mixed, gain, shift)).astype(bf16)

    def edge_part(layer, own):
        bias = ebias[layer : layer + 1, :]

        def body(t, carry):
            at = tile_at(t)
            total = 0.5 * (mm(edges[at, :], ein[layer, 0]) + bias)
            if own:
                total = total + mm(onehot[at, OWN:PLACES], table[OWN:PLACES, :])
            pre[at, :] = total
            return carry

        lax.fori_loop(0, tiles, body, 0)

    for get in get_vectors:
        get.wait()
    get_ein0.wait()
    project(0, OWN, hself[...])
    get_edges.wait()
    edge_part(0, True)
    out_far = []
    for i in range(CHUNKS):
        out_part[i].wait_recv()
        out_far.append(
            send(hpart.at[pl.ds(i * step, step)], hfar.at[pl.ds(i * step, step)], onward)
        )
        if i == HUB_TURN:
            hub_b = hub_gather(hub_a, hub_own, hub_got, hub_mid, hub_all)
    passed = out_far
    project(0, 0, hpart[...])
    gather(0, 2 * rows)
    hub_join(hub_b, hub_all, hub_rows)
    project_hub(0, hub_rows[...])
    for copy in out_far:
        copy.wait_recv()
    project(0, 2 * rows, hfar[...])
    get_eout.wait()
    update_edges(0, 2 * rows, OWN)

    size = rows // PIECES
    values = mm(scatter[0:rows, :], edges[...])
    self_send[...] = values.astype(bf16)
    sum_self[...] = values

    def send_self(i):
        return send(self_send.at[pl.ds(i * size, size)], self_in.at[pl.ds(i * size, size)], part)

    out_self = [send_self(i) for i in range(PIECES // 2)]
    values = mm(scatter[2 * rows : 3 * rows, :], edges[...])
    far_send[...] = values.astype(bf16)
    sum_far[...] = values
    sum_part[...] = mm(scatter[rows : 2 * rows, :], edges[...])
    zero_sum = jnp.zeros((HUB, dim), jnp.float32)
    hub_part = (
        jnp.where(owner1 == me, sum_self[0:HUB, :], zero_sum)
        + jnp.where(owner1 == part, sum_part[0:HUB, :], zero_sum)
        + jnp.where(owner1 == far, sum_far[0:HUB, :], zero_sum)
    ).astype(bf16)
    hub_cut(fub_own, hub_part)
    fub_a = hub_scatter(fub_own, fub_got)
    out_far = [
        send(far_send.at[pl.ds(i * size, size)], far_in.at[pl.ds(i * size, size)], source)
        for i in range(PIECES)
    ]
    out_self += [send_self(i) for i in range(PIECES // 2, PIECES)]
    get_ein1.wait()
    edge_part(1, False)
    aux_b = hub_gather(aux_a, aux_own, aux_got, aux_mid, aux_all)
    out_back = []
    out_pass = []
    for i in range(PIECES):
        at = pl.ds(i * size, size)
        mine = sum_part[at, :]
        out_far[i].wait_recv()
        from_far = far_in[at, :].astype(jnp.float32)
        back_send[at, :] = (mine + from_far).astype(bf16)
        sum_part[at, :] = mine + from_far
        out_back.append(send(back_send.at[at], back_in.at[at], part))
        out_self[i].wait_recv()
        from_part = self_in[at, :].astype(jnp.float32)
        pass_send[at, :] = (mine + from_part).astype(bf16)
        sum_part[at, :] = sum_part[at, :] + from_part
        out_pass.append(send(pass_send.at[at], pass_in.at[at], onward))
        if i == FUB_TURN:
            fub_b = hub_gather(fub_a, fub_own, fub_got, fub_mid, fub_all)
    get_nin.wait()
    get_nout.wait()
    for copy in passed:
        copy.wait_send()
    hpart[...] = update_nodes(0, hpart[...], sum_part[...].astype(bf16))
    project(1, 0, hpart[...])
    gather(0, 2 * rows)
    for copy in out_pass:
        copy.wait_recv()
    hfar_new = update_nodes(
        0, hfar[...], (sum_far[...] + pass_in[...].astype(jnp.float32)).astype(bf16)
    )
    project(1, 2 * rows, hfar_new)
    gather(2 * rows, 4 * rows)
    hub_join(aux_b, aux_all, aux_rows)
    hub_join(fub_b, fub_all, fub_rows)
    project_hub(1, update_nodes(0, aux_rows[...], fub_rows[...]))
    for copy in out_back:
        copy.wait_recv()
    hown = update_nodes(
        0, hself[...], (sum_self[...] + back_in[...].astype(jnp.float32)).astype(bf16)
    )
    project(1, OWN, hown)
    update_edges(1, HUB_AT, PLACES)

    values = mm(scatter[2 * rows : 3 * rows, :], edges[...])
    far_send2[...] = values.astype(bf16)
    sum_part[...] = mm(scatter[rows : 2 * rows, :], edges[...])
    out_far = [
        send(far_send2.at[pl.ds(i * size, size)], far_in2.at[pl.ds(i * size, size)], source)
        for i in range(PIECES)
    ]
    sum_self[...] = mm(scatter[0:rows, :], edges[...])
    out_back = []
    for i in range(PIECES):
        at = pl.ds(i * size, size)
        out_far[i].wait_recv()
        back_send2[at, :] = (sum_part[at, :] + far_in2[at, :].astype(jnp.float32)).astype(bf16)
        out_back.append(send(back_send2.at[at], back_in2.at[at], part))
    for copy in out_part:
        copy.wait_send()
    pltpu.make_async_copy(edges, edges_out, local_sems.at[7]).wait()
    puts = []
    for k in range(2):
        for copy in out_back[k * PIECES // 2 : (k + 1) * PIECES // 2]:
            copy.wait_recv()
        at = pl.ds(k * rows // 2, rows // 2)
        got = (sum_self[at, :] + back_in2[at, :].astype(jnp.float32)).astype(bf16)
        hself[at, :] = update_nodes(1, hown[k * rows // 2 : (k + 1) * rows // 2, :], got)
        puts.append(pltpu.make_async_copy(hself.at[at], nodes_out.at[at], local_sems.at[(8, 0)[k]]))
        puts[-1].start()
    for copy in sent:
        copy.wait_send()
    for put in puts:
        put.wait()


def copy_kernel(nodes, edges, nodes_out, edges_out, rows, lines, in_sems, out_sems):
    cut = lines.shape[0] // 4
    spans = [(nodes, nodes_out, rows, pl.ds(0, rows.shape[0]))]
    spans += [(edges, edges_out, lines, pl.ds(i * cut, cut)) for i in range(4)]
    gets = [
        pltpu.make_async_copy(src.at[at], held.at[at], in_sems.at[i])
        for i, (src, _, held, at) in enumerate(spans)
    ]
    puts = [
        pltpu.make_async_copy(held.at[at], dst.at[at], out_sems.at[i])
        for i, (_, dst, held, at) in enumerate(spans)
    ]
    for get in gets:
        get.start()
    for get, put in zip(gets, puts):
        get.wait()
        put.start()
    for put in puts:
        put.wait()


def copied(nodes, edges):
    hbm = pl.BlockSpec(memory_space=pl.ANY)
    return pl.pallas_call(
        copy_kernel,
        out_shape=(
            jax.ShapeDtypeStruct(nodes.shape, nodes.dtype),
            jax.ShapeDtypeStruct(edges.shape, edges.dtype),
        ),
        in_specs=[hbm, hbm],
        out_specs=(hbm, hbm),
        scratch_shapes=[
            pltpu.VMEM(nodes.shape, nodes.dtype),
            pltpu.VMEM(edges.shape, edges.dtype),
            pltpu.SemaphoreType.DMA((5,)),
            pltpu.SemaphoreType.DMA((5,)),
        ],
        compiler_params=pltpu.CompilerParams(vmem_limit_bytes=60 * 1024 * 1024),
        name="place",
    )(nodes, edges)


def local(
    nodes, edges, senders, receivers, valid_counts, hub_owner, edge_in, edge_bias, edge_out, edge_gain,
    edge_shift, node_in, node_bias, node_out, node_gain, node_shift,
):
    rows, dim = nodes.shape
    count = edges.shape[0]
    bf16 = jnp.bfloat16
    hub_owner = hub_owner.reshape(LAYERS)
    senders = senders.reshape(count // 128, 128)
    receivers = receivers.reshape(count // 128, 128)
    hbm = pl.BlockSpec(memory_space=pl.ANY)
    block = pltpu.VMEM((rows, dim), bf16)
    total = pltpu.VMEM((rows, dim), jnp.float32)

    def hub(pieces):
        return pltpu.VMEM((pieces, 2, 8, 128), bf16)

    hub_set = (hub(RUN), hub(N_PATCH - 1), hub(1), hub(RUN), pltpu.VMEM((HUB, dim), bf16))
    places = PLACES
    out = pl.pallas_call(
        kernel,
        out_shape=(
            jax.ShapeDtypeStruct((rows, dim), bf16),
            jax.ShapeDtypeStruct((count, dim), bf16),
        ),
        in_specs=[hbm] * 16,
        out_specs=(hbm, hbm),
        scratch_shapes=[
            block, block, block,
            pltpu.VMEM((count, dim), bf16),
            pltpu.VMEM((count, dim), jnp.float32),
            pltpu.VMEM((count, places), bf16),
            pltpu.VMEM((3 * rows, count), bf16),
            pltpu.VMEM((places, dim), bf16),
            pltpu.VMEM(edge_in.shape, bf16),
            pltpu.VMEM(edge_out.shape, bf16),
            pltpu.VMEM(node_in.shape, bf16),
            pltpu.VMEM(node_out.shape, bf16),
            total, total, total,
            *hub_set,
            *hub_set,
            *hub_set,
            pltpu.VMEM((TILE, dim), jnp.float32),
            pltpu.VMEM(senders.shape, jnp.int32),
            pltpu.VMEM(receivers.shape, jnp.int32),
            *([pltpu.VMEM(edge_bias.shape, jnp.float32)] * 6),
            pltpu.SMEM((1,), jnp.int32),
            pltpu.SMEM((LAYERS,), jnp.int32),
            block, block, block, block, block, block, block, block,
            block, block, block, block,
            pltpu.SemaphoreType.DMA((19,)),
            pltpu.SemaphoreType.DMA((144,)),
            pltpu.SemaphoreType.DMA((144,)),
        ],
        compiler_params=pltpu.CompilerParams(
            collective_id=0, has_side_effects=True, vmem_limit_bytes=60 * 1024 * 1024
        ),
        name="steps",
    )(
        nodes, edges, senders, receivers, valid_counts, hub_owner, edge_in, edge_bias, edge_out,
        edge_gain, edge_shift, node_in, node_bias, node_out, node_gain, node_shift,
    )
    return copied(*out)


def solution(mesh):
    split = P(GROUPS, None)
    line = P(GROUPS)
    return jax.shard_map(
        local,
        mesh=mesh,
        in_specs=(split, split, line, line, line, P(None, "region")) + (P(),) * 10,
        out_specs=(split, split),
        check_vma=False,
    )
```

```python
import functools

import jax
import jax.numpy as jnp
from jax import lax
from jax.experimental import pallas as pl
from jax.experimental.pallas import tpu as pltpu
from jax.sharding import PartitionSpec as P

HUB = 32
LAYERS = 2
GROUPS = ("region", "patch")
N_PATCH = 16
RUN = N_PATCH // 2
HUB_TURN = 3
FUB_TURN = 5
HUB_AT = 1024
OWN = 1152
PLACES = 1664
MESH = pl.DeviceIdType.MESH
EPS = 1e-05
TILE = 256
CHUNKS = 8
PIECES = 8


def flipped(index, mask):
    for bit in (1, 2, 4, 8):
        if mask & bit:
            index = index + bit - 2 * bit * ((index // bit) % 2)
    return index


class Trip:
    def __init__(self, copy):
        self.copy, self.left, self.landed = copy, False, False

    def wait_send(self):
        if not self.left:
            self.copy.wait_send()
        self.left = True

    def wait_recv(self):
        if not self.landed:
            self.copy.wait_recv()
        self.landed = True


def silu(half):
    return half + half * jnp.tanh(half)


def normed(value, gain, shift):
    share = 1.0 / value.shape[-1]
    center = value - jnp.sum(value, axis=-1, keepdims=True) * share
    spread = jnp.sum(center * center, axis=-1, keepdims=True) * share
    return center * lax.rsqrt(spread + EPS) * gain + shift


def mm(a, b):
    return jnp.dot(a, b, preferred_element_type=jnp.float32)


def kernel(
    nodes_hbm, edges_hbm, send_hbm, recv_hbm, valid_hbm, owner_hbm,
    ein_hbm, ebias_hbm, eout_hbm, egain_hbm, eshift_hbm, nin_hbm, nbias_hbm, nout_hbm, ngain_hbm, nshift_hbm,
    nodes_out, edges_out,
    hself, hpart, hfar, edges, pre, onehot, scatter, table,
    ein, eout, nin, nout,
    sum_self, sum_part, sum_far,
    hub_own, hub_got, hub_mid, hub_all, hub_rows,
    aux_own, aux_got, aux_mid, aux_all, aux_rows,
    fub_own, fub_got, fub_mid, fub_all, fub_rows,
    mixed_tile,
    send_codes, recv_codes, ebias, egain, eshift, nbias, ngain, nshift, valid_counts, hub_owner,
    self_send, self_in, far_send, far_in, back_send, back_in, pass_send, pass_in,
    far_send2, far_in2, back_send2, back_in2,
    local_sems, send_sems, recv_sems,
):
    rows = hself.shape[0]
    dim = hself.shape[1]
    count = edges.shape[0]
    tiles = count // TILE
    bf16 = jnp.bfloat16
    me = lax.axis_index("patch")
    region = lax.axis_index("region")
    odd = me % 2
    part = me + 1 - 2 * odd
    onward = (me + 2 - 4 * odd + N_PATCH) % N_PATCH
    source = (me - 2 + 4 * odd + N_PATCH) % N_PATCH
    far = (me - 1 + 2 * odd + N_PATCH) % N_PATCH

    barrier = pltpu.get_barrier_semaphore()
    others = [flipped(me, m) for m in range(1, N_PATCH)]
    greeted = [onward, source] + others
    for other in greeted:
        pl.semaphore_signal(barrier, inc=1, device_id=(region, other), device_id_type=MESH)

    def load(src, dst, index):
        copy = pltpu.make_async_copy(src, dst, local_sems.at[index])
        copy.start()
        return copy

    get_nodes = load(nodes_hbm, hself, 0)
    get_codes = [load(send_hbm, send_codes, 9), load(recv_hbm, recv_codes, 10)]
    get_codes += [load(owner_hbm, hub_owner, 11)]
    get_ein0 = load(ein_hbm.at[0], ein.at[0], 1)
    get_edges = load(edges_hbm, edges, 2)
    vectors = (
        (ebias_hbm, ebias), (egain_hbm, egain), (eshift_hbm, eshift), (nbias_hbm, nbias),
        (ngain_hbm, ngain), (nshift_hbm, nshift), (valid_hbm, valid_counts),
    )
    get_vectors = [load(src, dst, 12 + i) for i, (src, dst) in enumerate(vectors)]
    get_eout = load(eout_hbm, eout, 3)
    get_nin = load(nin_hbm, nin, 4)
    get_nout = load(nout_hbm, nout, 5)
    get_ein1 = load(ein_hbm.at[1], ein.at[1], 6)

    used = [0]

    def send(src, dst, other):
        index = used[0]
        used[0] += 1
        copy = pltpu.make_async_remote_copy(
            src, dst, send_sems.at[index], recv_sems.at[index],
            device_id=(region, other), device_id_type=MESH,
        )
        copy.start()
        trip = Trip(copy)
        sent.append(trip)
        return trip

    sent = []

    for get in get_codes:
        get.wait()
    codes = send_codes[...]
    is_odd = odd == 1
    behind = jnp.where(is_odd, codes, codes + 2 * rows)
    ahead = jnp.where(is_odd, codes, codes - 2 * rows)
    own = codes - rows + OWN
    send_pos = jnp.where(
        codes < rows, behind,
        jnp.where(codes < 2 * rows, own, jnp.where(codes < 3 * rows, ahead, codes + rows)),
    )
    rcodes = recv_codes[...]
    behind = jnp.where(is_odd, rcodes + rows, rcodes + 3 * rows)
    ahead = jnp.where(is_odd, rcodes + rows, rcodes - rows)
    recv_pos = jnp.where(rcodes < rows, behind, jnp.where(rcodes < 2 * rows, rcodes + OWN, ahead))
    behind = jnp.where(is_odd, rcodes + rows, rcodes + 2 * rows)
    ahead = jnp.where(is_odd, rcodes, rcodes - rows)
    add_pos = jnp.where(rcodes < rows, behind, jnp.where(rcodes < 2 * rows, rcodes - rows, ahead))
    block = 128
    lane = lax.broadcasted_iota(jnp.int32, (block, block), 1)
    line = lax.broadcasted_iota(jnp.int32, (3 * rows, block), 0)
    width = rows // block
    for b in range(count // block):
        send_col = jnp.broadcast_to(send_pos[b : b + 1, :], (block, block)).T
        recv_col = jnp.broadcast_to(recv_pos[b : b + 1, :], (block, block)).T
        starts = (0, rows, 2 * rows, 3 * rows, OWN, OWN + rows, HUB_AT)
        for seg, first in enumerate(starts):
            for w in range(width if seg < 6 else 1):
                start = first + w * block
                col = send_col if seg % 2 == 0 else recv_col
                onehot[b * block : (b + 1) * block, start : start + block] = jnp.where(
                    col == lane + start, 1.0, 0.0
                ).astype(bf16)
        scatter[:, b * block : (b + 1) * block] = jnp.where(
            add_pos[b : b + 1, :] == line, 1.0, 0.0
        ).astype(bf16)
    table[HUB_AT:OWN, :] = jnp.zeros((block, dim), bf16)

    def hub_cut(own, value):
        for piece in range(N_PATCH):
            r, c = divmod(piece, dim // 128)
            own[piece // 2, piece % 2] = value[r * 8 : (r + 1) * 8, c * 128 : (c + 1) * 128]

    get_nodes.wait()
    head = hself[0:HUB, :]
    owner0 = hub_owner[0]
    owner1 = hub_owner[1]
    zero_head = jnp.zeros_like(head)
    hub_cut(hub_own, jnp.where(owner0 == me, head, zero_head))
    hub_cut(aux_own, jnp.where(owner1 == me, head, zero_head))

    pl.semaphore_wait(barrier, len(greeted))

    def hub_scatter(own, got):
        return [send(own.at[other // 2], got.at[m], other) for m, other in enumerate(others)]

    def hub_gather(trips, own, got, mid, everyone):
        total = own[me // 2].astype(jnp.float32)
        for m, trip in enumerate(trips):
            trip.wait_recv()
            total = total + got[m].astype(jnp.float32)
        total = total.astype(bf16)
        mid[0] = total
        everyone[me // 2] = total
        return [send(mid.at[0], everyone.at[me // 2], other) for other in others[1::2]]

    def hub_join(trips, everyone, joined):
        for trip in trips:
            trip.wait_recv()
        for piece in range(N_PATCH):
            r, c = divmod(piece, dim // 128)
            joined[r * 8 : (r + 1) * 8, c * 128 : (c + 1) * 128] = everyone[piece // 2, piece % 2]

    step = rows // CHUNKS
    hub_a = hub_scatter(hub_own, hub_got)
    out_part = [
        send(hself.at[pl.ds(i * step, step)], hpart.at[pl.ds(i * step, step)], part)
        for i in range(CHUNKS)
    ]
    aux_a = hub_scatter(aux_own, aux_got)

    def project(layer, start, h):
        table[start : start + rows, :] = (0.5 * mm(h, ein[layer, 1])).astype(bf16)
        table[start + rows : start + 2 * rows, :] = (0.5 * mm(h, ein[layer, 2])).astype(bf16)

    def project_hub(layer, h):
        table[HUB_AT : HUB_AT + HUB, :] = (0.5 * mm(h, ein[layer, 1])).astype(bf16)

    def tile_at(t):
        return pl.ds(pl.multiple_of(t * TILE, TILE), TILE)

    def gather(low, high):
        def body(t, carry):
            at = tile_at(t)
            pre[at, :] += mm(onehot[at, low:high], table[low:high, :])
            return carry

        lax.fori_loop(0, tiles, body, 0)

    def update_edges(layer, low, high):
        valid = valid_counts[0]
        gain = egain[layer : layer + 1, :]
        shift = eshift[layer : layer + 1, :]

        def collect(t):
            at = tile_at(t)
            pre[at, :] += mm(onehot[at, low:high], table[low:high, :])

        def mix(t):
            mixed_tile[...] = mm(silu(pre[tile_at(t), :]).astype(bf16), eout[layer])

        def finish(t):
            at = tile_at(t)
            updated = edges[at, :].astype(jnp.float32) + normed(mixed_tile[...], gain, shift)
            row = lax.broadcasted_iota(jnp.int32, (TILE, 1), 0) + t * TILE
            edges[at, :] = jnp.where(row < valid, updated, 0.0).astype(bf16)
            if layer == LAYERS - 1:
                pltpu.make_async_copy(edges.at[at], edges_out.at[at], local_sems.at[7]).start()

        def body(t, carry):
            finish(t - 1)
            mix(t)
            collect(t + 1)
            return carry

        collect(0)
        mix(0)
        collect(1)
        lax.fori_loop(1, tiles - 1, body, 0)
        finish(tiles - 2)
        mix(tiles - 1)
        finish(tiles - 1)

    def update_nodes(layer, h, aggregate):
        total = mm(h, nin[layer, 0]) + mm(aggregate, nin[layer, 1]) + nbias[layer : layer + 1, :]
        mixed = mm(silu(0.5 * total).astype(bf16), nout[layer])
        gain = ngain[layer : layer + 1, :]
        shift = nshift[layer : layer + 1, :]
        return (h.astype(jnp.float32) + normed(mixed, gain, shift)).astype(bf16)

    def edge_part(layer, own):
        bias = ebias[layer : layer + 1, :]

        def body(t, carry):
            at = tile_at(t)
            total = 0.5 * (mm(edges[at, :], ein[layer, 0]) + bias)
            if own:
                total = total + mm(onehot[at, OWN:PLACES], table[OWN:PLACES, :])
            pre[at, :] = total
            return carry

        lax.fori_loop(0, tiles, body, 0)

    for get in get_vectors:
        get.wait()
    get_ein0.wait()
    project(0, OWN, hself[...])
    get_edges.wait()
    edge_part(0, True)
    out_far = []
    for i in range(CHUNKS):
        out_part[i].wait_recv()
        out_far.append(
            send(hpart.at[pl.ds(i * step, step)], hfar.at[pl.ds(i * step, step)], onward)
        )
        if i == HUB_TURN:
            hub_b = hub_gather(hub_a, hub_own, hub_got, hub_mid, hub_all)
    passed = out_far
    project(0, 0, hpart[...])
    gather(0, 2 * rows)
    hub_join(hub_b, hub_all, hub_rows)
    project_hub(0, hub_rows[...])
    for copy in out_far:
        copy.wait_recv()
    project(0, 2 * rows, hfar[...])
    get_eout.wait()
    update_edges(0, 2 * rows, OWN)

    size = rows // PIECES
    values = mm(scatter[0:rows, :], edges[...])
    self_send[...] = values.astype(bf16)
    sum_self[...] = values

    def send_self(i):
        return send(self_send.at[pl.ds(i * size, size)], self_in.at[pl.ds(i * size, size)], part)

    out_self = [send_self(i) for i in range(PIECES // 2)]
    values = mm(scatter[2 * rows : 3 * rows, :], edges[...])
    far_send[...] = values.astype(bf16)
    sum_far[...] = values
    sum_part[...] = mm(scatter[rows : 2 * rows, :], edges[...])
    zero_sum = jnp.zeros((HUB, dim), jnp.float32)
    hub_part = (
        jnp.where(owner1 == me, sum_self[0:HUB, :], zero_sum)
        + jnp.where(owner1 == part, sum_part[0:HUB, :], zero_sum)
        + jnp.where(owner1 == far, sum_far[0:HUB, :], zero_sum)
    ).astype(bf16)
    hub_cut(fub_own, hub_part)
    fub_a = hub_scatter(fub_own, fub_got)
    out_far = [
        send(far_send.at[pl.ds(i * size, size)], far_in.at[pl.ds(i * size, size)], source)
        for i in range(PIECES)
    ]
    out_self += [send_self(i) for i in range(PIECES // 2, PIECES)]
    get_ein1.wait()
    edge_part(1, False)
    aux_b = hub_gather(aux_a, aux_own, aux_got, aux_mid, aux_all)
    out_back = []
    out_pass = []
    for i in range(PIECES):
        at = pl.ds(i * size, size)
        mine = sum_part[at, :]
        out_far[i].wait_recv()
        from_far = far_in[at, :].astype(jnp.float32)
        back_send[at, :] = (mine + from_far).astype(bf16)
        sum_part[at, :] = mine + from_far
        out_back.append(send(back_send.at[at], back_in.at[at], part))
        out_self[i].wait_recv()
        from_part = self_in[at, :].astype(jnp.float32)
        pass_send[at, :] = (mine + from_part).astype(bf16)
        sum_part[at, :] = sum_part[at, :] + from_part
        out_pass.append(send(pass_send.at[at], pass_in.at[at], onward))
        if i == FUB_TURN:
            fub_b = hub_gather(fub_a, fub_own, fub_got, fub_mid, fub_all)
    get_nin.wait()
    get_nout.wait()
    for copy in passed:
        copy.wait_send()
    hpart[...] = update_nodes(0, hpart[...], sum_part[...].astype(bf16))
    project(1, 0, hpart[...])
    gather(0, 2 * rows)
    for copy in out_pass:
        copy.wait_recv()
    hfar_new = update_nodes(
        0, hfar[...], (sum_far[...] + pass_in[...].astype(jnp.float32)).astype(bf16)
    )
    project(1, 2 * rows, hfar_new)
    gather(2 * rows, 4 * rows)
    hub_join(aux_b, aux_all, aux_rows)
    hub_join(fub_b, fub_all, fub_rows)
    project_hub(1, update_nodes(0, aux_rows[...], fub_rows[...]))
    for copy in out_back:
        copy.wait_recv()
    hown = update_nodes(
        0, hself[...], (sum_self[...] + back_in[...].astype(jnp.float32)).astype(bf16)
    )
    project(1, OWN, hown)
    update_edges(1, HUB_AT, PLACES)

    values = mm(scatter[2 * rows : 3 * rows, :], edges[...])
    far_send2[...] = values.astype(bf16)
    earlier = list(sent)
    out_far = [
        send(far_send2.at[pl.ds(i * size, size)], far_in2.at[pl.ds(i * size, size)], source)
        for i in range(PIECES)
    ]
    sum_part[...] = mm(scatter[rows : 2 * rows, :], edges[...])
    sum_self[...] = mm(scatter[0:rows, :], edges[...])
    for copy in earlier:
        copy.wait_send()
    pltpu.make_async_copy(edges, edges_out, local_sems.at[7]).wait()
    out_back = []
    for i in range(PIECES):
        at = pl.ds(i * size, size)
        out_far[i].wait_recv()
        back_send2[at, :] = (sum_part[at, :] + far_in2[at, :].astype(jnp.float32)).astype(bf16)
        out_back.append(send(back_send2.at[at], back_in2.at[at], part))
    puts = []
    for k in range(2):
        for copy in out_back[k * PIECES // 2 : (k + 1) * PIECES // 2]:
            copy.wait_recv()
        at = pl.ds(k * rows // 2, rows // 2)
        got = (sum_self[at, :] + back_in2[at, :].astype(jnp.float32)).astype(bf16)
        hself[at, :] = update_nodes(1, hown[k * rows // 2 : (k + 1) * rows // 2, :], got)
        puts.append(pltpu.make_async_copy(hself.at[at], nodes_out.at[at], local_sems.at[(8, 0)[k]]))
        puts[-1].start()
    for copy in sent:
        copy.wait_send()
    for put in puts:
        put.wait()


def copy_kernel(nodes, edges, nodes_out, edges_out, rows, lines, in_sems, out_sems):
    cut = lines.shape[0] // 8
    spans = [(nodes, nodes_out, rows, pl.ds(0, rows.shape[0]))]
    spans += [(edges, edges_out, lines, pl.ds(i * cut, cut)) for i in range(8)]
    gets = [
        pltpu.make_async_copy(src.at[at], held.at[at], in_sems.at[i])
        for i, (src, _, held, at) in enumerate(spans)
    ]
    puts = [
        pltpu.make_async_copy(held.at[at], dst.at[at], out_sems.at[i])
        for i, (_, dst, held, at) in enumerate(spans)
    ]
    for get in gets:
        get.start()
    for get, put in zip(gets, puts):
        get.wait()
        put.start()
    for put in puts:
        put.wait()


def copied(nodes, edges):
    hbm = pl.BlockSpec(memory_space=pl.ANY)
    return pl.pallas_call(
        copy_kernel,
        out_shape=(
            jax.ShapeDtypeStruct(nodes.shape, nodes.dtype),
            jax.ShapeDtypeStruct(edges.shape, edges.dtype),
        ),
        in_specs=[hbm, hbm],
        out_specs=(hbm, hbm),
        scratch_shapes=[
            pltpu.VMEM(nodes.shape, nodes.dtype),
            pltpu.VMEM(edges.shape, edges.dtype),
            pltpu.SemaphoreType.DMA((9,)),
            pltpu.SemaphoreType.DMA((9,)),
        ],
        compiler_params=pltpu.CompilerParams(vmem_limit_bytes=60 * 1024 * 1024),
        name="place",
    )(nodes, edges)


def local(
    nodes, edges, senders, receivers, valid_counts, hub_owner, edge_in, edge_bias, edge_out, edge_gain,
    edge_shift, node_in, node_bias, node_out, node_gain, node_shift,
):
    rows, dim = nodes.shape
    count = edges.shape[0]
    bf16 = jnp.bfloat16
    hub_owner = hub_owner.reshape(LAYERS)
    senders = senders.reshape(count // 128, 128)
    receivers = receivers.reshape(count // 128, 128)
    hbm = pl.BlockSpec(memory_space=pl.ANY)
    block = pltpu.VMEM((rows, dim), bf16)
    total = pltpu.VMEM((rows, dim), jnp.float32)

    def hub(pieces):
        return pltpu.VMEM((pieces, 2, 8, 128), bf16)

    hub_set = (hub(RUN), hub(N_PATCH - 1), hub(1), hub(RUN), pltpu.VMEM((HUB, dim), bf16))
    places = PLACES
    out = pl.pallas_call(
        kernel,
        out_shape=(
            jax.ShapeDtypeStruct((rows, dim), bf16),
            jax.ShapeDtypeStruct((count, dim), bf16),
        ),
        in_specs=[hbm] * 16,
        out_specs=(hbm, hbm),
        scratch_shapes=[
            block, block, block,
            pltpu.VMEM((count, dim), bf16),
            pltpu.VMEM((count, dim), jnp.float32),
            pltpu.VMEM((count, places), bf16),
            pltpu.VMEM((3 * rows, count), bf16),
            pltpu.VMEM((places, dim), bf16),
            pltpu.VMEM(edge_in.shape, bf16),
            pltpu.VMEM(edge_out.shape, bf16),
            pltpu.VMEM(node_in.shape, bf16),
            pltpu.VMEM(node_out.shape, bf16),
            total, total, total,
            *hub_set,
            *hub_set,
            *hub_set,
            pltpu.VMEM((TILE, dim), jnp.float32),
            pltpu.VMEM(senders.shape, jnp.int32),
            pltpu.VMEM(receivers.shape, jnp.int32),
            *([pltpu.VMEM(edge_bias.shape, jnp.float32)] * 6),
            pltpu.SMEM((1,), jnp.int32),
            pltpu.SMEM((LAYERS,), jnp.int32),
            block, block, block, block, block, block, block, block,
            block, block, block, block,
            pltpu.SemaphoreType.DMA((19,)),
            pltpu.SemaphoreType.DMA((144,)),
            pltpu.SemaphoreType.DMA((144,)),
        ],
        compiler_params=pltpu.CompilerParams(
            collective_id=0, has_side_effects=True, vmem_limit_bytes=60 * 1024 * 1024
        ),
        name="steps",
    )(
        nodes, edges, senders, receivers, valid_counts, hub_owner, edge_in, edge_bias, edge_out,
        edge_gain, edge_shift, node_in, node_bias, node_out, node_gain, node_shift,
    )
    return copied(*out)


def solution(mesh):
    split = P(GROUPS, None)
    line = P(GROUPS)
    return jax.shard_map(
        local,
        mesh=mesh,
        in_specs=(split, split, line, line, line, P(None, "region")) + (P(),) * 10,
        out_specs=(split, split),
        check_vma=False,
    )
```
